32 devices in a mesh: row: 8 (over y, x, core), col: 4 (over z).
Axes of the slice: x: 2, y: 2, z: 4, core: 2. Of those that a mesh axis runs over, the one named last changes fastest.
Arguments:
- features: bfloat16 [65536, 256], P(('col', 'row')), may hold values from -6 to 6
- block_values: bfloat16 [8, 4, 192, 128, 128], P('row', 'col'), may hold values from -0.1875 to 0.1875
- row_ptr: int32 [8, 4, 65], P('row', 'col'), may hold values from 0 to 144, as said below
- block_cols: int32 [8, 4, 192], P('row', 'col'), may hold values from 0 to 511, as said below
Outputs:
- product: bfloat16 [65536, 256], P(('row', 'col'))
The draws below stay inside these ranges and needn't reach their ends.
Inputs may be any that keep to these rules, and one draw needn't show every extreme that they name: row_ptr[r, c, 0] = 0, row_ptr never falls along its last dimension, row_ptr[r, c, 64] <= 144, and on exactly one device row_ptr[r, c, 64] = 144. block_cols[r, c, s] lies in c * 128 to (c + 1) * 128 - 1; a block column may repeat within a block row, and repeated blocks add.
All inputs are finite; a program needn't handle non-finite values.
Results may differ from the reference program's by a relative error of at most 0.001.
Values may be sent and summed in bfloat16 or wider, within the bound.
A program may use at most 128 MiB of HBM per device.

```python
import jax
import jax.numpy as jnp
from jax import lax

B = 128
NCOL = 256
BR = 64
SLOTS = 192
NB = 512
BC = 128
N_ROW = 8
N_COL = 4


def pattern(key):
    key_fill = jax.random.fold_in(key, 11)
    key_busy = jax.random.fold_in(key, 12)
    key_rows = jax.random.fold_in(key, 13)
    key_cols = jax.random.fold_in(key, 14)
    filled = SLOTS // 8 + jax.random.randint(key_fill, (N_ROW, N_COL), 0, SLOTS // 4 + 1)
    busiest = jax.random.randint(key_busy, (), 0, N_ROW * N_COL)
    position = jnp.arange(N_ROW * N_COL, dtype=jnp.int32).reshape(N_ROW, N_COL)
    filled = jnp.where(position == busiest, 3 * SLOTS // 4, filled)
    slot_ids = jnp.arange(SLOTS, dtype=jnp.int32)
    rows = jax.random.randint(key_rows, (N_ROW, N_COL, SLOTS), 0, BR)
    rows = jnp.where(slot_ids[None, None, :] < filled[:, :, None], rows, BR)
    bounds = jnp.arange(BR + 1, dtype=jnp.int32)
    pointers = jnp.sum((rows[:, :, None, :] < bounds[None, None, :, None]).astype(jnp.int32), axis=-1)
    group_start = (jnp.arange(N_COL, dtype=jnp.int32) * BC)[None, :, None]
    columns = jax.random.randint(key_cols, (N_ROW, N_COL, SLOTS), 0, BC) + group_start
    return (pointers.astype(jnp.int32), columns.astype(jnp.int32))


def draw_row_ptr(key, part):
    pointers, columns = pattern(key)
    return pointers


def draw_block_cols(key, part):
    pointers, columns = pattern(key)
    return columns


def level_of(rng, shape, pieces, low, top_value):
    gain = 1.0
    for dim, shards_of in pieces:
        heights = jax.random.uniform(jax.random.fold_in(jax.random.fold_in(rng, 6), dim), (shards_of,), jnp.float32, low / len(pieces), top_value / len(pieces))
        gain = gain * jnp.repeat(jnp.exp(heights), shape[dim] // shards_of).reshape((-1,) + (1,) * (len(shape) - 1 - dim))
    return gain


def scatter_about(rng, dims, scale, most, split=(), kind=jnp.bfloat16):
    array = scale * jax.random.normal(rng, dims, jnp.float32)
    if split:
        array = array * level_of(rng, dims, split, -0.22, 0.18)
    return jnp.clip(array, -most, most).astype(kind)


def setup_inputs(seed: int = 0) -> dict:
    seeds = jax.random.split(jax.random.key(seed), 5)
    features = scatter_about(seeds[0], (NB * B, NCOL), 1.0, 6.0, ((0, 32),))
    block_values = scatter_about(seeds[1], (N_ROW, N_COL, SLOTS, B, B), (9 * B) ** -0.5, 0.1875, ((0, 8), (1, 4)))
    row_ptr = draw_row_ptr(jax.random.fold_in(seeds[4], 71), 0)
    block_cols = draw_block_cols(jax.random.fold_in(seeds[4], 71), 0)
    return dict(features=features, block_values=block_values, row_ptr=row_ptr, block_cols=block_cols)


def row_weights(pointers, slot_count):
    slot_ids = jnp.arange(slot_count, dtype=jnp.int32)
    inside = (pointers[:-1, None] <= slot_ids[None, :]) & (slot_ids[None, :] < pointers[1:, None])
    return inside.astype(jnp.float32)


def reference(features, block_values, row_ptr, block_cols):
    block_size = block_values.shape[-1]
    panel = features.reshape(-1, block_size, features.shape[1])

    def one_group(operands):
        values_row, pointers_row, columns_row = operands

        def add_device(running, device_ops):
            values, pointers, columns = device_ops
            blocks = panel[columns.astype(jnp.int32)].astype(jnp.float32)
            products = jnp.einsum("sij,sjk->sik", values.astype(jnp.float32), blocks, precision=lax.Precision.HIGHEST)
            weights = row_weights(pointers.astype(jnp.int32), values.shape[0])
            summed = jnp.einsum("rs,sik->rik", weights, products, precision=lax.Precision.HIGHEST)
            return running + summed, jnp.zeros((), jnp.float32)

        starting = jnp.zeros((row_ptr.shape[2] - 1, block_size, features.shape[1]), jnp.float32)
        running, unused = lax.scan(add_device, starting, (values_row, pointers_row, columns_row))
        return running

    groups = lax.map(one_group, (block_values, row_ptr, block_cols))
    return groups.reshape(features.shape[0], features.shape[1]).astype(jnp.bfloat16)
```

```python
import functools

import jax
import jax.numpy as jnp
from jax import lax
from jax.experimental import pallas as pl
from jax.experimental.pallas import tpu as pltpu
from jax.sharding import PartitionSpec as P

LANES = 128
TOP = 32767.0
RIGHT, LEFT = 0, 1


def kernel(
    n_row, n_col, cols, keep, last, filled, features, values_hbm, out,
    panels, values, sums, send_q, recv_q, send_s, recv_s,
    local_sem, ag_send, ag_recv, pair_send, pair_recv, rs_send, rs_recv, sc_send, sc_recv,
):
    n_chips = n_row // 2
    own_blocks = features.shape[0]
    chunks = len(panels)
    live = values.shape[0]
    shard = out.shape[0]
    r, c = lax.axis_index("row"), lax.axis_index("col")
    chip, core = r // 2, r % 2
    partner = chip * 2 + 1 - core

    def slot(k, row):
        return panels[k].at[pl.ds(row * own_blocks, own_blocks)]

    own = [
        pltpu.make_async_copy(
            features.at[:, :, pl.ds(k * LANES, LANES)], slot(k, r), local_sem.at[k]
        )
        for k in range(chunks)
    ]
    for copy in own:
        copy.start()
    fetch = pltpu.make_async_copy(
        values_hbm.at[0, 0, pl.ds(0, live)], values, local_sem.at[chunks]
    )
    fetch.start()

    barrier = pltpu.get_barrier_semaphore()

    def greet(**where):
        pl.semaphore_signal(
            barrier, inc=1, device_id=where, device_id_type=pl.DeviceIdType.MESH
        )

    for o in range(1, n_chips):
        greet(row=((chip + o) % n_chips) * 2 + core)
    greet(row=partner)
    pl.when(c > 0)(lambda: greet(col=c - 1))
    pl.when(c < n_col - 1)(lambda: greet(col=c + 1))
    ends = jnp.where(c > 0, 1, 0) + jnp.where(c < n_col - 1, 1, 0)
    pl.semaphore_wait(barrier, n_chips + ends)

    def remote(src, dst, send, recv, **where):
        return pltpu.make_async_remote_copy(
            src_ref=src, dst_ref=dst, send_sem=send, recv_sem=recv,
            device_id=where, device_id_type=pl.DeviceIdType.MESH,
        )

    def across(k, o):
        target = ((chip + o) % n_chips) * 2 + core
        return remote(slot(k, r), slot(k, r), ag_send.at[k, o], ag_recv.at[k, o], row=target)

    def arriving(k, o):
        row = ((chip + n_chips - o) % n_chips) * 2 + core
        return remote(slot(k, row), slot(k, row), ag_send.at[k, o], ag_recv.at[k, o], row=row)

    def pair(k, o):
        row = ((chip + n_chips - o) % n_chips) * 2 + core
        return remote(slot(k, row), slot(k, row), pair_send.at[k, o], pair_recv.at[k, o], row=partner)

    def pair_arriving(k, o):
        row = ((chip + n_chips - o) % n_chips) * 2 + 1 - core
        return remote(slot(k, row), slot(k, row), pair_send.at[k, o], pair_recv.at[k, o], row=partner)

    def gather_start(k):
        own[k].wait()
        for o in range(1, n_chips):
            across(k, o).start()
        pair(k, 0).start()

    def gather_finish(k):
        for o in range(1, n_chips):
            arriving(k, o).wait_recv()
            pair(k, o).start()
        for o in range(n_chips):
            pair_arriving(k, o).wait_recv()

    unroll = 4 if live % 4 == 0 else 1

    def compute(k):
        def step(i, total):
            first = i * unroll
            products = [
                jnp.dot(
                    values[first + u], panels[k][cols[first + u]],
                    preferred_element_type=jnp.float32,
                )
                for u in range(unroll)
            ]
            for u in range(unroll):
                total = total * keep[first + u] + products[u]
                sums[k, first + u] = total
            return total

        lax.fori_loop(0, live // unroll, step, jnp.zeros(sums.shape[2:], jnp.float32))

    def row_sum(k, q):
        return sums[k, last[q]] * filled[q]

    def received(way, k, j, b):
        levels = recv_q[way, k, j, b].astype(jnp.int32).astype(jnp.float32)
        return levels * recv_s[way, k, j, pl.ds(b, 1), :]

    def message(way, k, j):
        to = c + 1 if way == RIGHT else c - 1
        return (
            remote(send_q.at[way, k, j], recv_q.at[way, k, j],
                   rs_send.at[way, k, j], rs_recv.at[way, k, j], col=to),
            remote(send_s.at[way, k, j], recv_s.at[way, k, j],
                   sc_send.at[way, k, j], sc_recv.at[way, k, j], col=to),
        )

    def forward(way, k, j, incoming):
        if incoming:
            for copy in message(way, k, j):
                copy.wait_recv()

        def one(b, carry):
            x = row_sum(k, j * shard + b)
            if incoming:
                x = x + received(way, k, j, b)
            most = jnp.maximum(jnp.max(jnp.abs(x), axis=0, keepdims=True), 1e-30)
            send_s[way, k, j, pl.ds(b, 1), :] = most * (1.0 / TOP)
            send_q[way, k, j, b] = jnp.round(x * (TOP / most)).astype(jnp.int32).astype(jnp.int16)
            return carry

        lax.fori_loop(0, shard, one, 0)
        for copy in message(way, k, j):
            copy.start()

    def scatter_ends(k):
        @pl.when(c == 0)
        def _():
            for j in range(n_col - 1, 0, -1):
                forward(RIGHT, k, j, False)

        @pl.when(c == n_col - 1)
        def _():
            for j in range(n_col - 1):
                forward(LEFT, k, j, False)

    def scatter_step(k, u):
        right = n_col - 1 - u + c
        left = u - (n_col - 1 - c)

        @pl.when((c > 0) & (right <= n_col - 1) & (right > c))
        def _():
            forward(RIGHT, k, right, True)

        @pl.when((c < n_col - 1) & (left >= 0) & (left < c))
        def _():
            forward(LEFT, k, left, True)

    def finish(k):
        def write(ways):
            for way in ways:
                for copy in message(way, k, c):
                    copy.wait_recv()

            def one(b, carry):
                x = row_sum(k, c * shard + b)
                for way in ways:
                    x = x + received(way, k, c, b)
                out[b, :, pl.ds(k * LANES, LANES)] = x.astype(out.dtype)
                return carry

            lax.fori_loop(0, shard, one, 0)

        pl.when(c == 0)(lambda: write((LEFT,)))
        pl.when(c == n_col - 1)(lambda: write((RIGHT,)))
        pl.when((c > 0) & (c < n_col - 1))(lambda: write((RIGHT, LEFT)))

    gather_start(0)
    fetch.wait()
    gather_finish(0)
    for k in range(chunks):
        if k + 1 < chunks:
            gather_start(k + 1)
        compute(k)
        scatter_ends(k)
        if k > 0:
            for u in range(2, n_col - 1):
                scatter_step(k - 1, u)
            finish(k - 1)
        scatter_step(k, 1)
        if k + 1 < chunks:
            gather_finish(k + 1)
    for u in range(2, n_col - 1):
        scatter_step(chunks - 1, u)
    finish(chunks - 1)

    for k in range(chunks):
        for o in range(n_chips):
            if o > 0:
                across(k, o).wait_send()
            pair(k, o).wait_send()
        for j in range(n_col):
            for way, sent in ((RIGHT, c < j), (LEFT, c > j)):
                @pl.when(sent)
                def _(way=way, k=k, j=j):
                    for copy in message(way, k, j):
                        copy.wait_send()


def local(n_row, n_col, features, block_values, row_ptr, block_cols):
    pointers = row_ptr[0, 0]
    slots, block = block_values.shape[2], block_values.shape[3]
    live = slots * 3 // 4
    rows = pointers.shape[0] - 1
    own_blocks = features.shape[0] // block
    group_blocks = own_blocks * n_row
    chunks = features.shape[1] // LANES
    shard = rows // n_col
    cols = block_cols[0, 0] - lax.axis_index("col") * group_blocks
    ids = jnp.arange(slots, dtype=jnp.int32)
    begins = jnp.any(pointers[:, None] == ids[None, :], axis=0)
    keep = jnp.where(begins, 0.0, 1.0).astype(jnp.float32)
    last = jnp.maximum(pointers[1:] - 1, 0)
    filled = (pointers[1:] > pointers[:-1]).astype(jnp.float32)
    smem = pl.BlockSpec(memory_space=pltpu.SMEM)
    hbm = pl.BlockSpec(memory_space=pl.ANY)
    messages = (2, chunks, n_col)
    result = pl.pallas_call(
        functools.partial(kernel, n_row, n_col),
        out_shape=jax.ShapeDtypeStruct((shard, block, features.shape[1]), jnp.bfloat16),
        in_specs=[smem] * 4 + [hbm] * 2,
        out_specs=pl.BlockSpec(memory_space=pltpu.VMEM),
        scratch_shapes=[
            [pltpu.VMEM((group_blocks, block, LANES), jnp.bfloat16)] * chunks,
            pltpu.VMEM((live, block, block), jnp.bfloat16),
            pltpu.VMEM((chunks, live, block, LANES), jnp.float32),
            pltpu.VMEM(messages + (shard, block, LANES), jnp.int16),
            pltpu.VMEM(messages + (shard, block, LANES), jnp.int16),
            pltpu.VMEM(messages + (shard, LANES), jnp.float32),
            pltpu.VMEM(messages + (shard, LANES), jnp.float32),
            pltpu.SemaphoreType.DMA((chunks + 1,)),
            pltpu.SemaphoreType.DMA((chunks, n_row // 2)),
            pltpu.SemaphoreType.DMA((chunks, n_row // 2)),
            pltpu.SemaphoreType.DMA((chunks, n_row // 2)),
            pltpu.SemaphoreType.DMA((chunks, n_row // 2)),
            pltpu.SemaphoreType.DMA(messages),
            pltpu.SemaphoreType.DMA(messages),
            pltpu.SemaphoreType.DMA(messages),
            pltpu.SemaphoreType.DMA(messages),
        ],
        compiler_params=pltpu.CompilerParams(
            collective_id=0, has_side_effects=True, vmem_limit_bytes=67043328
        ),
    )(cols, keep, last, filled, features.reshape(own_blocks, block, -1), block_values)
    return result.reshape(shard * block, -1)


def solution(mesh):
    return jax.shard_map(
        functools.partial(local, mesh.shape["row"], mesh.shape["col"]),
        mesh=mesh,
        in_specs=(
            P(("col", "row"), None),
            P("row", "col", None, None, None),
            P("row", "col", None),
            P("row", "col", None),
        ),
        out_specs=P(("row", "col"), None),
        check_vma=False,
    )
```

```python
import functools

import jax
import jax.numpy as jnp
from jax import lax
from jax.experimental import pallas as pl
from jax.experimental.pallas import tpu as pltpu
from jax.sharding import PartitionSpec as P

LANES = 128
TOP = 32767.0
RIGHT, LEFT = 0, 1


def kernel(
    n_row, n_col, pointers, block_cols, features, values_hbm, out,
    panels, values, keep, sums, send_q, recv_q, send_s, recv_s,
    local_sem, ag_send, ag_recv, pair_send, pair_recv, rs_send, rs_recv, sc_send, sc_recv,
):
    n_chips = n_row // 2
    own_blocks = features.shape[0]
    half = own_blocks // 2
    chunks = len(panels)
    live = values.shape[0]
    shard = out.shape[0]
    parts, width = send_s.shape[3], send_s.shape[4]
    r, c = lax.axis_index("row"), lax.axis_index("col")
    chip, core = r // 2, r % 2
    square = n_chips == 4
    first_block = c * (own_blocks * n_row)

    def chip_to(o):
        if square:
            y, x = chip // 2, chip % 2
            return (1 - y if o >= 2 else y) * 2 + (1 - x if o % 2 else x)
        return (chip + o) % n_chips

    def chip_from(o):
        return chip_to(o) if square else (chip + n_chips - o) % n_chips

    partner = chip * 2 + 1 - core
    direct = (1, 2) if square else tuple(range(1, n_chips))

    def slot(k, row, h):
        return panels[k].at[pl.ds(row * own_blocks + h * half, half)]

    own = [
        pltpu.make_async_copy(
            features.at[:, :, pl.ds(k * LANES, LANES)],
            panels[k].at[pl.ds(r * own_blocks, own_blocks)],
            local_sem.at[k],
        )
        for k in range(chunks)
    ]
    for copy in own:
        copy.start()
    fetch = pltpu.make_async_copy(
        values_hbm.at[0, 0, pl.ds(0, live)], values, local_sem.at[chunks]
    )
    fetch.start()

    barrier = pltpu.get_barrier_semaphore()

    def greet(**where):
        pl.semaphore_signal(
            barrier, inc=1, device_id=where, device_id_type=pl.DeviceIdType.MESH
        )

    for o in direct:
        greet(row=chip_to(o) * 2 + core)
    greet(row=partner)
    pl.when(c > 0)(lambda: greet(col=c - 1))
    pl.when(c < n_col - 1)(lambda: greet(col=c + 1))
    ends = jnp.where(c > 0, 1, 0) + jnp.where(c < n_col - 1, 1, 0)
    pl.semaphore_wait(barrier, len(direct) + 1 + ends)

    def remote(src, dst, send, recv, **where):
        return pltpu.make_async_remote_copy(
            src_ref=src, dst_ref=dst, send_sem=send, recv_sem=recv,
            device_id=where, device_id_type=pl.DeviceIdType.MESH,
        )

    def piece(k, o, h, source, to):
        return remote(
            slot(k, source * 2 + core, h), slot(k, source * 2 + core, h),
            ag_send.at[k, o, h], ag_recv.at[k, o, h], row=to * 2 + core,
        )

    def across(k, o, h):
        return piece(k, o, h, chip, chip_to(o))

    def arriving(k, o, h):
        return piece(k, o, h, chip_from(o), chip_from(o))

    def relay(k, h):
        return piece(k, 3, h, chip_from(1 + h), chip_to(2 - h))

    def pair(k, o, h, whose):
        row = (chip_from(o) if o else chip) * 2 + whose
        return remote(
            slot(k, row, h), slot(k, row, h), pair_send.at[k, o, h], pair_recv.at[k, o, h],
            row=partner,
        )

    if square:
        order = ((1, 0), (2, 1), (1, 1), (2, 0))
    else:
        order = tuple((o, h) for o in direct for h in range(2))

    def gather_start(k):
        own[k].wait()
        for o, h in order:
            across(k, o, h).start()
        for h in range(2):
            pair(k, 0, h, core).start()

    def gather_finish(k):
        for o, h in order:
            arriving(k, o, h).wait_recv()
            if square and (o, h) in ((1, 0), (2, 1)):
                relay(k, h).start()
            pair(k, o, h, core).start()
        if square:
            for h in range(2):
                arriving(k, 3, h).wait_recv()
                pair(k, 3, h, core).start()
        for o in range(n_chips):
            for h in range(2):
                pair(k, o, h, 1 - core).wait_recv()

    unroll = 4 if live % 4 == 0 else 1

    def mark_rows():
        ids = lax.broadcasted_iota(jnp.int32, keep.shape, 0)

        def mark(q, flags):
            return jnp.where(ids == pointers[0, 0, q], 0.0, flags)

        keep[...] = lax.fori_loop(0, pointers.shape[2], mark, jnp.ones(keep.shape, jnp.float32))

    def compute(k):
        def step(i, total):
            first = i * unroll
            products = [
                jnp.dot(
                    values[first + u], panels[k][jnp.maximum(block_cols[0, 0, first + u] - first_block, 0)],
                    preferred_element_type=jnp.float32,
                )
                for u in range(unroll)
            ]
            for u in range(unroll):
                total = total * keep[pl.ds(first + u, 1), :] + products[u]
                sums[k, first + u] = total
            return total

        lax.fori_loop(0, live // unroll, step, jnp.zeros(sums.shape[2:], jnp.float32))

    def row_sum(k, q):
        begin, end = pointers[0, 0, q], pointers[0, 0, q + 1]
        return sums[k, jnp.maximum(end - 1, 0)] * jnp.where(end > begin, 1.0, 0.0)

    def received(way, k, j, s, b):
        levels = recv_q[way, k, j, s * width + b].astype(jnp.int32).astype(jnp.float32)
        return levels * recv_s[way, k, j, s, pl.ds(b, 1), :]

    def message(way, k, j, s):
        to = c + 1 if way == RIGHT else c - 1
        rows = pl.ds(s * width, width)
        return (
            remote(send_q.at[way, k, j, rows], recv_q.at[way, k, j, rows],
                   rs_send.at[way, k, j, s], rs_recv.at[way, k, j, s], col=to),
            remote(send_s.at[way, k, j, s], recv_s.at[way, k, j, s],
                   sc_send.at[way, k, j, s], sc_recv.at[way, k, j, s], col=to),
        )

    def forward(way, k, j, s, incoming):
        if incoming:
            for copy in message(way, k, j, s):
                copy.wait_recv()

        def one(b, carry):
            x = row_sum(k, j * shard + s * width + b)
            if incoming:
                x = x + received(way, k, j, s, b)
            most = jnp.maximum(jnp.max(jnp.abs(x), axis=0, keepdims=True), 1e-30)
            send_s[way, k, j, s, pl.ds(b, 1), :] = most * (1.0 / TOP)
            levels = jnp.round(x * (TOP / most)).astype(jnp.int32)
            send_q[way, k, j, s * width + b] = levels.astype(jnp.int16)
            return carry

        lax.fori_loop(0, width, one, 0)
        for copy in message(way, k, j, s):
            copy.start()

    def scatter_ends(k):
        def right(m, carry):
            forward(RIGHT, k, n_col - 1 - m // parts, m % parts, False)
            return carry

        def left(m, carry):
            forward(LEFT, k, m // parts, m % parts, False)
            return carry

        total = (n_col - 1) * parts

        @pl.when(c == 0)
        def _():
            lax.fori_loop(0, total, right, 0)

        @pl.when(c == n_col - 1)
        def _():
            lax.fori_loop(0, total, left, 0)

    def scatter_middle(k):
        def unit(n, carry):
            right = n - c
            left = n - (n_col - 1 - c)

            @pl.when((c > 0) & (right >= 0) & (right < (n_col - 1 - c) * parts))
            def _():
                forward(RIGHT, k, n_col - 1 - right // parts, right % parts, True)

            @pl.when((c < n_col - 1) & (left >= 0) & (left < c * parts))
            def _():
                forward(LEFT, k, left // parts, left % parts, True)

            return carry

        lax.fori_loop(1, (n_col - 2) * parts + 1, unit, 0)

    def finish(k):
        def write(ways):
            def part(s, carry):
                for way in ways:
                    for copy in message(way, k, c, s):
                        copy.wait_recv()

                def one(b, inner):
                    x = row_sum(k, c * shard + s * width + b)
                    for way in ways:
                        x = x + received(way, k, c, s, b)
                    out[s * width + b, :, pl.ds(k * LANES, LANES)] = x.astype(out.dtype)
                    return inner

                return lax.fori_loop(0, width, one, carry)

            lax.fori_loop(0, parts, part, 0)

        pl.when(c == 0)(lambda: write((LEFT,)))
        pl.when(c == n_col - 1)(lambda: write((RIGHT,)))
        pl.when((c > 0) & (c < n_col - 1))(lambda: write((RIGHT, LEFT)))

    gather_start(0)
    mark_rows()
    fetch.wait()
    gather_finish(0)
    for k in range(chunks):
        if k + 1 < chunks:
            gather_start(k + 1)
        compute(k)
        scatter_ends(k)
        if k > 0:
            scatter_middle(k - 1)
            finish(k - 1)
        if k + 1 < chunks:
            gather_finish(k + 1)
    scatter_middle(chunks - 1)
    finish(chunks - 1)

    for k in range(chunks):
        for h in range(2):
            for o in direct:
                across(k, o, h).wait_send()
            if square:
                relay(k, h).wait_send()
            for o in range(n_chips):
                pair(k, o, h, core).wait_send()
        for way in (RIGHT, LEFT):
            def drain(m, carry, way=way, k=k):
                j = m // parts

                @pl.when((j > c) if way == RIGHT else (j < c))
                def _():
                    for copy in message(way, k, j, m % parts):
                        copy.wait_send()

                return carry

            lax.fori_loop(0, n_col * parts, drain, 0)


def local(n_row, n_col, features, block_values, row_ptr, block_cols):
    slots, block = block_values.shape[2], block_values.shape[3]
    live = slots * 3 // 4
    own_blocks = features.shape[0] // block
    group_blocks = own_blocks * n_row
    chunks = features.shape[1] // LANES
    shard = (row_ptr.shape[2] - 1) // n_col
    parts = 4 if shard % 4 == 0 else 1
    smem = pl.BlockSpec(memory_space=pltpu.SMEM)
    hbm = pl.BlockSpec(memory_space=pl.ANY)
    messages = (2, chunks, n_col)
    gathers = (chunks, n_row // 2, 2)
    result = pl.pallas_call(
        functools.partial(kernel, n_row, n_col),
        out_shape=jax.ShapeDtypeStruct((shard, block, features.shape[1]), jnp.bfloat16),
        in_specs=[smem] * 2 + [hbm] * 2,
        out_specs=pl.BlockSpec(memory_space=pltpu.VMEM),
        scratch_shapes=[
            [pltpu.VMEM((group_blocks, block, LANES), jnp.bfloat16)] * chunks,
            pltpu.VMEM((live, block, block), jnp.bfloat16),
            pltpu.VMEM((live, LANES), jnp.float32),
            pltpu.VMEM((chunks, live, block, LANES), jnp.float32),
            pltpu.VMEM(messages + (shard, block, LANES), jnp.int16),
            pltpu.VMEM(messages + (shard, block, LANES), jnp.int16),
            pltpu.VMEM(messages + (parts, shard // parts, LANES), jnp.float32),
            pltpu.VMEM(messages + (parts, shard // parts, LANES), jnp.float32),
            pltpu.SemaphoreType.DMA((chunks + 1,)),
        ]
        + [pltpu.SemaphoreType.DMA(gathers)] * 4
        + [pltpu.SemaphoreType.DMA(messages + (parts,))] * 4,
        compiler_params=pltpu.CompilerParams(
            collective_id=0, has_side_effects=True, vmem_limit_bytes=67043328
        ),
    )(row_ptr, block_cols, features.reshape(own_blocks, block, -1), block_values)
    return result.reshape(shard * block, -1)


def solution(mesh):
    return jax.shard_map(
        functools.partial(local, mesh.shape["row"], mesh.shape["col"]),
        mesh=mesh,
        in_specs=(
            P(("col", "row"), None),
            P("row", "col", None, None, None),
            P("row", "col", None),
            P("row", "col", None),
        ),
        out_specs=P(("row", "col"), None),
        check_vma=False,
    )
```
